32 devices in a mesh: gx: 8 (over z, y), gy: 4 (over x, core).
Axes of the slice: x: 2, y: 2, z: 4, core: 2. Of those that a mesh axis runs over, the one named last changes fastest.
Arguments:
- charge_density: float32 [256, 256, 256], P('gx', 'gy'), may hold values from -5080 to 5140
Outputs:
- potential: float32 [256, 256, 256], P('gx', 'gy')
- energies: float32 [2], replicated
The draws below stay inside these ranges and needn't reach their ends.
All inputs are finite; a program needn't handle non-finite values.
Results may differ from the reference program's by a relative error of at most 0.0003.
Values sent between devices are 32-bit elements.
A program may use at most 192 MiB of HBM per device.

```python
import math
import jax
import jax.numpy as jnp
import numpy as np
from jax import lax

N = 256
ORDER = 16


def draw_charge_density(key, part):
    level_key, noise_key = jax.random.split(jax.random.fold_in(key, 11))
    bound = float((N + 1) * (N + 1) // 13)
    levels = jax.random.uniform(level_key, (8, 8, 8), jnp.float32, minval=0.0, maxval=60.0)
    noise = jax.random.uniform(noise_key, (N, N, N), jnp.float32, minval=-bound, maxval=bound)
    block = N // 8
    coarse = jnp.repeat(jnp.repeat(jnp.repeat(levels, block, 0), block, 1), block, 2)
    return (coarse + noise).astype(jnp.float32)


def setup_inputs(seed: int = 0) -> dict:
    key_of = jax.random.split(jax.random.key(seed), 2)
    return {
        "charge_density": draw_charge_density(jax.random.fold_in(key_of[1], 71), 0),
    }


exact_mode = lax.Precision.HIGHEST
outer_ratio = 1.1
radius_scale = math.sqrt(3.0) / 2.0

def sine_table(length):
    counter = jnp.arange(length, dtype=jnp.int32) + 1
    product = counter[:, None] * counter[None, :] % (2 * (length + 1))
    return jnp.sin(math.pi * product.astype(jnp.float32) / (length + 1))

def eigen_line(counter, length):
    half_angle = math.pi * (counter + 1).astype(jnp.float32) / (2.0 * (length + 1))
    return 4.0 * float((length + 1) * (length + 1)) * jnp.sin(half_angle) ** 2

def recurrence_tables():
    degree_count = ORDER + 1
    near_coeff = np.zeros((degree_count, degree_count, 1), np.float32)
    far_coeff = np.zeros((degree_count, degree_count, 1), np.float32)
    sector = np.ones(degree_count, np.float32)
    for degree in range(1, degree_count):
        for azimuth in range(degree):
            divisor = math.sqrt(degree * degree - azimuth * azimuth)
            near_coeff[degree, azimuth, 0] = (2 * degree - 1) / divisor
            far_coeff[degree, azimuth, 0] = math.sqrt((degree - 1) * (degree - 1) - azimuth * azimuth) / divisor
        if degree >= 2:
            sector[degree] = math.sqrt((2 * degree - 1) / (2.0 * degree))
    return (near_coeff, far_coeff, sector)

def expansion_weights():
    degree_count = ORDER + 1
    weights = np.zeros((degree_count, degree_count), np.float32)
    for degree in range(degree_count):
        for azimuth in range(degree + 1):
            factor = 1.0 if azimuth == 0 else 2.0
            weights[degree, azimuth] = factor / (4.0 * math.pi * radius_scale * outer_ratio ** (degree + 1))
    return weights

def harmonic_sweep(unit_x, unit_y, unit_z, visitor, running):
    near_coeff, far_coeff, sector = recurrence_tables()
    degree_count = ORDER + 1
    selector = np.eye(degree_count, dtype=np.float32)[:, :, None]
    empty_rows = jnp.zeros((degree_count,) + unit_x.shape, unit_x.dtype)
    sector_cosine = jnp.ones_like(unit_x)
    sector_sine = jnp.zeros_like(unit_x)
    cosine_prev, sine_prev, cosine_old, sine_old = (empty_rows, empty_rows, empty_rows, empty_rows)
    for degree in range(degree_count):
        if degree > 0:
            sector_cosine, sector_sine = (sector[degree] * (unit_x * sector_cosine - unit_y * sector_sine), sector[degree] * (unit_x * sector_sine + unit_y * sector_cosine))
        cosine_now = near_coeff[degree] * unit_z * cosine_prev - far_coeff[degree] * cosine_old + selector[degree] * sector_cosine
        sine_now = near_coeff[degree] * unit_z * sine_prev - far_coeff[degree] * sine_old + selector[degree] * sector_sine
        running = visitor(running, degree, cosine_now, sine_now)
        cosine_old, sine_old = (cosine_prev, sine_prev)
        cosine_prev, sine_prev = (cosine_now, sine_now)
    return running

def face_moments(point_x, point_y, point_z, charge):
    radius = jnp.sqrt(point_x * point_x + point_y * point_y + point_z * point_z)
    scaled_radius = radius / radius_scale

    def visitor(running, degree, cosine_now, sine_now):
        weight, moment_cosine, moment_sine, facing_cosine, facing_sine = running
        moment_cosine = moment_cosine + [jnp.dot(cosine_now, weight, precision=exact_mode)]
        moment_sine = moment_sine + [jnp.dot(sine_now, weight, precision=exact_mode)]
        facing_cosine = facing_cosine + [jnp.dot(cosine_now, charge, precision=exact_mode)]
        facing_sine = facing_sine + [jnp.dot(sine_now, charge, precision=exact_mode)]
        return (weight * scaled_radius, moment_cosine, moment_sine, facing_cosine, facing_sine)
    result = harmonic_sweep(point_x / radius, point_y / radius, point_z / radius, visitor, (charge, [], [], [], []))
    return tuple((jnp.stack(listing) for listing in result[1:]))

def face_potential(point_x, point_y, point_z, weight_cosine, weight_sine):
    radius = jnp.sqrt(point_x * point_x + point_y * point_y + point_z * point_z)

    def visitor(accum, degree, cosine_now, sine_now):
        accum = accum + jnp.dot(weight_cosine[degree], cosine_now, precision=exact_mode)
        return accum + jnp.dot(weight_sine[degree], sine_now, precision=exact_mode)
    return harmonic_sweep(point_x / radius, point_y / radius, point_z / radius, visitor, jnp.zeros_like(point_x))

def transform(volume, sine_rows):
    volume = jnp.einsum('abc,ck->abk', volume, sine_rows, precision=exact_mode)
    volume = jnp.einsum('abk,bj->ajk', volume, sine_rows, precision=exact_mode)
    return jnp.einsum('ajk,ai->ijk', volume, sine_rows, precision=exact_mode)

def poisson_solve(volume, sine_rows, denominator):
    return transform(transform(volume, sine_rows) / denominator, sine_rows)

def reference(charge_density):
    length = N
    spacing = 1.0 / (length + 1)
    sine_rows = sine_table(length)
    eigen_rows = eigen_line(jnp.arange(length, dtype=jnp.int32), length)
    denominator = (eigen_rows[:, None, None] + eigen_rows[None, :, None] + eigen_rows[None, None, :]) * ((length + 1) / 2.0) ** 3
    first_field = poisson_solve(charge_density, sine_rows, denominator)
    coords = (jnp.arange(length, dtype=jnp.float32) - (length - 1) / 2.0) * spacing
    grid_rows = jnp.broadcast_to(coords[:, None], (length, length)).reshape(-1)
    grid_columns = jnp.broadcast_to(coords[None, :], (length, length)).reshape(-1)
    plane_half = jnp.full((length * length,), 0.5, jnp.float32)
    boundary_faces = [(grid_rows, grid_columns, -plane_half, first_field[:, :, 0]), (grid_rows, grid_columns, plane_half, first_field[:, :, -1]), (-plane_half, grid_rows, grid_columns, first_field[0]), (plane_half, grid_rows, grid_columns, first_field[-1]), (grid_rows, -plane_half, grid_columns, first_field[:, 0]), (grid_rows, plane_half, grid_columns, first_field[:, -1])]
    totals = None
    for point_x, point_y, point_z, near_cells in boundary_faces:
        face_terms = face_moments(point_x, point_y, point_z, spacing * near_cells.reshape(-1))
        if totals is None:
            totals = face_terms
        else:
            totals = tuple((earlier + later for earlier, later in zip(totals, face_terms)))
    weights = expansion_weights()
    weight_cosine = weights * totals[0]
    weight_sine = weights * totals[1]
    potentials = []
    for point_x, point_y, point_z, near_cells in boundary_faces:
        potentials.append(face_potential(point_x, point_y, point_z, weight_cosine, weight_sine).reshape(length, length) / spacing ** 2)
    source = charge_density
    source = source.at[:, :, 0].add(potentials[0])
    source = source.at[:, :, -1].add(potentials[1])
    source = source.at[0].add(potentials[2])
    source = source.at[-1].add(potentials[3])
    source = source.at[:, 0].add(potentials[4])
    source = source.at[:, -1].add(potentials[5])
    potential = poisson_solve(source, sine_rows, denominator)
    energies = spacing ** 3 * jnp.stack([jnp.sum(charge_density * first_field), jnp.sum(charge_density * potential)])
    return (potential, energies)
```

```python
import functools
import math

import jax
import jax.numpy as jnp
import numpy as np
from jax import lax
from jax.experimental import pallas as pl
from jax.experimental.pallas import tpu as pltpu
from jax.sharding import PartitionSpec as P

ORDER = 16
DEG = ORDER + 1
RATIO = 1.1
RADIUS = math.sqrt(3.0) / 2.0
HIGH = lax.Precision.HIGH
BEST = lax.Precision.HIGHEST


def solid_harmonics(x, y, z):
    rr = x * x + y * y + z * z
    out = np.zeros((DEG, 2 * DEG - 1) + x.shape)
    cos = np.zeros((DEG, DEG) + x.shape)
    sin = np.zeros((DEG, DEG) + x.shape)
    cos[0, 0] = 1.0
    for l in range(1, DEG):
        s = 1.0 if l == 1 else math.sqrt((2 * l - 1) / (2.0 * l))
        cos[l, l] = s * (x * cos[l - 1, l - 1] - y * sin[l - 1, l - 1])
        sin[l, l] = s * (x * sin[l - 1, l - 1] + y * cos[l - 1, l - 1])
        for m in range(l):
            div = math.sqrt(l * l - m * m)
            far = math.sqrt((l - 1) * (l - 1) - m * m) if l - 1 > m else 0.0
            for f in (cos, sin):
                f[l, m] = (2 * l - 1) * z * f[l - 1, m] / div
                if l >= 2 and far:
                    f[l, m] = f[l, m] - far * rr * f[l - 2, m] / div
    out[:, :DEG] = cos
    out[:, DEG:] = sin[:, 1:]
    return out


def face_tensors():
    t = np.cos(np.pi * (np.arange(DEG) + 0.5) / DEG)
    fwd = np.cos(np.arange(DEG)[:, None] * np.arccos(t)[None, :]) * (2.0 / DEG)
    fwd[0] *= 0.5
    u, v = np.meshgrid(t / 2, t / 2, indexing="ij")
    half = np.full_like(u, 0.5)
    tensors = []
    for pts in ((half, u, v), (u, half, v), (u, v, half)):
        vals = solid_harmonics(*pts)
        tensors.append(np.einsum("pu,lfuv,qv->lfpq", fwd, vals, fwd))
    par = np.ones((3, DEG, 2 * DEG - 1))
    for l in range(DEG):
        for f in range(2 * DEG - 1):
            m, odd = (f, 0) if f < DEG else (f - ORDER, 1)
            par[0, l, f] = (-1.0) ** (m + odd)
            par[1, l, f] = (-1.0) ** odd
            par[2, l, f] = (-1.0) ** (l + m)
    return np.stack(tensors).astype(np.float32).reshape(3, DEG, 2 * DEG - 1, DEG * DEG), par.astype(np.float32)


def expansion_weights():
    w = np.zeros((DEG, 2 * DEG - 1))
    for l in range(DEG):
        for f in range(2 * DEG - 1):
            m = f if f < DEG else f - ORDER
            w[l, f] = (1.0 if m == 0 else 2.0) / (4.0 * math.pi * RADIUS * RATIO ** (l + 1))
    return w.astype(np.float32)


def edges_kernel(v_ref, lam_ref, left_ref, right_ref):
    lam = lam_ref[...]
    m = v_ref.shape[0]
    left = v_ref[0]
    right = v_ref[m - 1]
    for i in range(1, m):
        left = left * lam + v_ref[i]
        right = right * lam + v_ref[m - 1 - i]
    left_ref[...] = left
    right_ref[...] = right


def solve_kernel(v_ref, lam_ref, inv_ref, a_ref, b_ref, w_ref):
    lam = lam_ref[...]
    inv = inv_ref[...]
    m = v_ref.shape[0]
    carry = b_ref[...]
    for i in range(m - 1, -1, -1):
        carry = carry * lam
        w_ref[i] = carry
        carry = carry + v_ref[i]
    carry = a_ref[...]
    for i in range(m):
        carry = carry * lam + v_ref[i]
        w_ref[i] = (carry + w_ref[i]) * inv


def block_edges(v, lam, rows):
    m, n, width = v.shape
    plane = pl.BlockSpec((rows, width), lambda j: (j, 0))
    return pl.pallas_call(
        edges_kernel,
        grid=(n // rows,),
        in_specs=[pl.BlockSpec((m, rows, width), lambda j: (0, j, 0)), plane],
        out_specs=[plane, plane],
        out_shape=[jax.ShapeDtypeStruct((n, width), jnp.float32)] * 2,
    )(v, lam)


def block_solve(v, lam, inv, a, b, rows):
    m, n, width = v.shape
    plane = pl.BlockSpec((rows, width), lambda j: (j, 0))
    cube = pl.BlockSpec((m, rows, width), lambda j: (0, j, 0))
    return pl.pallas_call(
        solve_kernel,
        grid=(n // rows,),
        in_specs=[cube, plane, plane, plane, plane],
        out_specs=cube,
        out_shape=jax.ShapeDtypeStruct(v.shape, jnp.float32),
    )(v, lam, inv, a, b)


def shards(charge_density):
    ca, cb, n = charge_density.shape
    gx, gy = lax.axis_size("gx"), lax.axis_size("gy")
    ix, iy = lax.axis_index("gx"), lax.axis_index("gy")
    kb = n // gy
    pack = max(1, 128 // kb)
    while ca % pack:
        pack //= 2
    sub = ca // pack
    width = pack * kb
    h = 1.0 / (n + 1)
    norm = (2.0 * h) ** 2

    num = np.arange(n) + 1
    sine64 = np.sin(np.pi * ((num[:, None] * num[None, :]) % (2 * (n + 1))) / (n + 1))
    sine = jnp.asarray(sine64.astype(np.float32))
    eps64 = 4.0 * np.sin(np.pi * num / (2.0 * (n + 1))) ** 2
    cheb64 = np.cos(np.arange(DEG)[None, :] * np.arccos((2.0 * np.arange(n) - (n - 1)) * h)[:, None])
    cheb = jnp.asarray(cheb64.astype(np.float32))
    chebhat = jnp.asarray((sine64 @ cheb64).astype(np.float32))
    tensors, parity = face_tensors()

    eps = jnp.asarray(eps64.astype(np.float32))
    eps_k = lax.dynamic_slice_in_dim(eps, iy * kb, kb)
    sigma = eps[:, None] + eps_k[None, :]
    s = 0.5 * jnp.sqrt(sigma)
    t = jnp.sqrt(1.0 + s * s)
    theta = 2.0 * jnp.log1p(s + s * s / (1.0 + t))
    lam_k = jnp.exp(-theta)
    inv_k = 1.0 / (4.0 * s * t)

    def power(e):
        return jnp.exp(-theta * e)

    lam = jnp.tile(lam_k, (1, pack))
    inv = jnp.tile(inv_k, (1, pack))
    rows = min(n, 64)
    det = 1.0 / (1.0 - power(2.0 * (n + 1)))
    lam_sub = power(float(sub))
    lam_blk = power(float(ca))

    def exchange(v):
        left, right = block_edges(v, lam, rows)
        left = [left[:, g * kb : (g + 1) * kb] for g in range(pack)]
        right = [right[:, g * kb : (g + 1) * kb] for g in range(pack)]
        dev_l, dev_r = left[0], right[pack - 1]
        for g in range(1, pack):
            dev_l = dev_l * lam_sub + left[g]
            dev_r = dev_r * lam_sub + right[pack - 1 - g]
        both = lax.all_gather(jnp.concatenate([dev_l, dev_r], axis=1), "gx")
        all_l, all_r = both[:, :, :kb], both[:, :, kb:]
        tot_l = jnp.zeros_like(dev_l)
        tot_r = jnp.zeros_like(dev_l)
        in_l = jnp.zeros_like(dev_l)
        in_r = jnp.zeros_like(dev_l)
        for p in range(gx):
            tot_l = tot_l * lam_blk + all_l[p]
            tot_r = tot_r * lam_blk + all_r[gx - 1 - p]
            in_l = jnp.where(p < ix, in_l * lam_blk + all_l[p], in_l)
            in_r = jnp.where(gx - 1 - p > ix, in_r * lam_blk + all_r[gx - 1 - p], in_r)
        f0 = lam_k * tot_r * det
        f1 = lam_k * tot_l * det
        base = (ix * ca).astype(jnp.float32)
        carry_l, carry_r = [in_l], [in_r]
        for g in range(pack - 1):
            carry_l.append(carry_l[-1] * lam_sub + left[g])
            carry_r.append(carry_r[-1] * lam_sub + right[pack - 1 - g])
        carry_r = carry_r[::-1]
        a_parts, b_parts = [], []
        for g in range(pack):
            at = base + float(g * sub)
            a_parts.append(carry_l[g] - (f0 * power(at) - f1 * power(n + 1 + at)))
            b_parts.append(
                carry_r[g]
                + (f0 * power(2.0 * (n + 1) - at - sub - 1) - f1 * power(n - at - sub))
            )
        return jnp.concatenate(a_parts, axis=1), jnp.concatenate(b_parts, axis=1)

    def solve(v):
        a, b = exchange(v)
        return block_solve(v, lam, inv, a, b, rows)

    spec = jnp.einsum("abz,zk->abk", charge_density, sine, precision=HIGH)
    spec = spec.reshape(pack, sub, cb, gy, kb).transpose(3, 1, 2, 0, 4).reshape(gy, sub, cb, width)
    spec = lax.all_to_all(spec, "gy", split_axis=0, concat_axis=0, tiled=True)
    spec = spec.transpose(1, 0, 2, 3).reshape(sub, n, width)
    sine_h2 = jnp.asarray((sine64 * h * h).astype(np.float32))
    rhs = jnp.einsum("jb,sbl->sjl", sine_h2, spec, precision=HIGH)

    first = solve(rhs)

    edge_rows = jnp.stack([sine[0], sine[n - 1]])
    edge_k = lax.dynamic_slice_in_dim(edge_rows, iy * kb, kb, 1)
    hat_k = lax.dynamic_slice_in_dim(chebhat, iy * kb, kb, 0)
    cheb_a = lax.dynamic_slice_in_dim(cheb, ix * ca, ca, 0)
    wall_x = jnp.stack([first[0, :, :kb], first[sub - 1, :, width - kb :]])
    own_x = jnp.stack([ix == 0, ix == gx - 1]).astype(jnp.float32)
    wall_x = wall_x * own_x[:, None, None]
    mom_x = jnp.einsum("fjk,jp->fpk", wall_x, chebhat, precision=BEST)
    mom_x = jnp.einsum("fpk,kq->fpq", mom_x, hat_k, precision=BEST)
    wall_y = jnp.sum(first[None] * edge_rows[:, None, :, None], axis=2)
    wall_y = wall_y.reshape(2, sub, pack, kb).transpose(0, 2, 1, 3).reshape(2, ca, kb)
    mom_y = jnp.einsum("fak,ap->fpk", wall_y, cheb_a, precision=BEST)
    mom_y = jnp.einsum("fpk,kq->fpq", mom_y, hat_k, precision=BEST)
    edge_lane = jnp.einsum("fk,gh->gkfh", edge_k, jnp.eye(pack, dtype=jnp.float32)).reshape(width, 2 * pack)
    wall_z = jnp.einsum("sjl,lc->csj", first, edge_lane, precision=HIGH)
    wall_z = wall_z.reshape(2, ca, n)
    mom_z = jnp.einsum("faj,jq->faq", wall_z, chebhat, precision=BEST)
    mom_z = jnp.einsum("faq,ap->fpq", mom_z, cheb_a, precision=BEST)
    moments = jnp.stack([mom_x, mom_y, mom_z]).reshape(-1) * (h * norm)
    energy_one = h * norm * jnp.sum(first * rhs)
    packed = jnp.concatenate([moments, energy_one[None]])
    packed = jnp.sum(lax.all_gather(packed, ("gx", "gy")), axis=0)
    moments = packed[:-1].reshape(3, 2, 1, 1, DEG * DEG)
    energy_one = packed[-1]

    tens = jnp.asarray(tensors)
    par = jnp.asarray(parity)
    gain = jnp.asarray(expansion_weights() * (RADIUS ** -np.arange(DEG, dtype=np.float64))[:, None].astype(np.float32))
    lm = jnp.sum(tens * moments[:, 1], axis=3) + par * jnp.sum(tens * moments[:, 0], axis=3)
    lm = jnp.sum(lm, axis=0) * gain
    coef_hi = jnp.sum(tens * lm[None, :, :, None], axis=2).reshape(3, DEG, DEG, DEG)
    coef_lo = jnp.sum(tens * (par * lm[None])[..., None], axis=2).reshape(3, DEG, DEG, DEG)

    coord = jnp.asarray(((np.arange(n) - (n - 1) / 2.0) * h).astype(np.float32))
    coord_a = lax.dynamic_slice_in_dim(coord, ix * ca, ca)

    def face(coefs, cheb_u, cheb_v, u, v):
        part = jnp.einsum("flpq,up->fluq", coefs, cheb_u, precision=BEST)
        part = jnp.einsum("fluq,vq->fluv", part, cheb_v, precision=HIGH)
        rinv = lax.rsqrt(0.25 + u[:, None] * u[:, None] + v[None, :] * v[None, :])
        acc = part[:, ORDER]
        for l in range(ORDER - 1, -1, -1):
            acc = acc * rinv + part[:, l]
        return acc

    coef_x = jnp.where(ix == 0, coef_lo[0], coef_hi[0])[None]
    phi_x = face(coef_x, cheb, cheb, coord, coord)[0]
    phi_y = face(jnp.stack([coef_lo[1], coef_hi[1]]), cheb_a, cheb, coord_a, coord)
    phi_z = face(jnp.stack([coef_lo[2], coef_hi[2]]), cheb_a, cheb, coord_a, coord)

    sine_k = lax.dynamic_slice_in_dim(sine, iy * kb, kb, 1)
    hat_x = jnp.einsum("yz,zk->yk", phi_x, sine_k, precision=HIGH)
    hat_x = jnp.einsum("jy,yk->jk", sine, hat_x, precision=HIGH)
    hat_y = jnp.einsum("faz,zk->fak", phi_y, sine_k, precision=HIGH)
    hat_z = jnp.einsum("fay,yj->faj", phi_z, sine, precision=HIGH)
    hat_y = hat_y.reshape(2, pack, sub, kb).transpose(0, 2, 1, 3).reshape(2, sub, 1, width)
    add = hat_y[0] * edge_rows[0][None, :, None] + hat_y[1] * edge_rows[1][None, :, None]
    add = add + jnp.einsum(
        "csj,lc->sjl", hat_z.reshape(2 * pack, sub, n), edge_lane, precision=HIGH
    )
    rhs2 = rhs + add
    blank = jnp.zeros((n, width - kb), jnp.float32)
    rhs2 = rhs2.at[0].add(own_x[0] * jnp.concatenate([hat_x, blank], axis=1))
    rhs2 = rhs2.at[sub - 1].add(own_x[1] * jnp.concatenate([blank, hat_x], axis=1))
    energy_two = h * norm * jnp.sum(first * rhs2)
    energy_two = jnp.sum(lax.all_gather(energy_two, ("gx", "gy")))

    second = solve(rhs2)
    back = jnp.asarray((sine64 * norm).astype(np.float32)).reshape(gy, cb, n)
    out = jnp.einsum("pbj,sjl->psbl", back, second, precision=HIGH)
    out = lax.all_to_all(out, "gy", split_axis=0, concat_axis=0, tiled=True)
    out = out.reshape(gy, sub, cb, pack, kb).transpose(3, 1, 2, 0, 4).reshape(ca, cb, n)
    potential = jnp.einsum("abk,kz->abz", out, sine, precision=HIGH)
    return potential, jnp.stack([energy_one, energy_two])


def solution(mesh):
    return jax.shard_map(
        shards,
        mesh=mesh,
        in_specs=(P("gx", "gy", None),),
        out_specs=(P("gx", "gy", None), P()),
        check_vma=False,
    )
```
